32 devices in a mesh: grp: 2 (over x), seq: 16 (over z, y, core).
Axes of the slice: x: 2, y: 2, z: 4, core: 2. Of those that a mesh axis runs over, the one named last changes fastest.
Arguments:
- queries: bfloat16 [512, 4096], P(('grp', 'seq')), parts along dimension 0, may hold values from -36 to 36
- new_keys: bfloat16 [512, 1024], P(('grp', 'seq')), parts along dimension 0, may hold values from -24 to 24
- new_values: bfloat16 [512, 1024], P(('grp', 'seq')), parts along dimension 0, may hold values from -12 to 12
- suffix_keys: bfloat16 [512, 256, 1024], P(('grp', 'seq')), parts along dimension 0, may hold values from -18 to 18
- suffix_values: bfloat16 [512, 256, 1024], P(('grp', 'seq')), parts along dimension 0, may hold values from -12 to 12
- suffix_lens: int32 [512], P(('grp', 'seq')), parts along dimension 0, may hold values from 1 to 256, 32768 in all
- prefix_keys: bfloat16 [2048, 16, 1024], P(('grp', 'seq')), parts along dimension 0, may hold values from -12 to 12
- prefix_values: bfloat16 [2048, 16, 1024], P(('grp', 'seq')), parts along dimension 0, may hold values from -12 to 12
- page_table: int32 [4, 512], P('grp'), parts along dimension 0, may hold values from 0 to 1023, as said below
- prefix_id: int32 [512], P('grp'), parts along dimension 0, may hold values from 0 to 1
Outputs:
- attn_out: bfloat16 [512, 4096], P(('grp', 'seq')), parts along dimension 0
The draws below stay inside these ranges and needn't reach their ends.
There are 2 independent parts, one for each index of `grp`. The reference program is written for one: setup_inputs(seed, part) draws one part's arguments, and reference() takes and returns one part's arrays. A program takes and returns all parts, laid end to end along the dimension named above; each array names one. Nothing has to cross between parts.
Inputs may be any that keep to these rules, and one draw needn't show every extreme that they name: `page_table`: every page id 0 to 1023 stands exactly once in the table. Each run of 64 page ids that starts at a multiple of 64 holds at least one page of every prefix.
All inputs are finite; a program needn't handle non-finite values. No bound on the sum of `suffix_lens` on one device may be relied on, other than what follows from the above.
Results may differ from the reference program's by a relative error of at most 0.005.
Values may be sent and summed in bfloat16 or wider, within the bound.
A program may use at most 192 MiB of HBM per device.

```python
import math
import jax
import jax.numpy as jnp
import numpy as np
from jax import lax

H = 32
KV = 8
HD = 128
NPREF = 2
PAGE = 16
PAGES_DEV = 64
B_DEV = 16
SUF = 256
B = 256
PAGES = 1024
PPP = 512
N_SEQ = 16


def shared_keys(key):
    raw_keys = 4.0 * jax.random.normal(jax.random.fold_in(key, 11), (B, KV * HD), jnp.float32)
    return jnp.clip(raw_keys, -24.0, 24.0)


def draw_new_keys(key, part):
    return shared_keys(key).astype(jnp.bfloat16)


def draw_queries(key, part):
    plain_draw = jnp.clip(jax.random.normal(jax.random.fold_in(key, 12), (B, H * HD), jnp.float32), -6.0, 6.0)
    return plain_draw.astype(jnp.bfloat16)


def draw_page_table(key, part):
    owner_count = PAGES // PAGES_DEV
    spare_slots = PAGES_DEV - NPREF
    leftover = jnp.repeat(jnp.arange(NPREF, dtype=jnp.int32), PPP - owner_count)
    leftover = jax.random.permutation(jax.random.fold_in(key, 3), leftover).reshape(owner_count, spare_slots)
    base_rows = jnp.tile(jnp.arange(NPREF, dtype=jnp.int32)[None, :], (owner_count, 1))
    labels = jnp.concatenate([base_rows, leftover], axis=1)
    labels = jax.random.permutation(jax.random.fold_in(key, 4), labels, axis=1, independent=True)
    order_list = jnp.argsort(labels.reshape(-1), stable=True)
    return order_list.reshape(NPREF, PPP).astype(jnp.int32)


def set_ends(drawn, stream_key, smallest, high):
    dims = drawn.shape
    spot = [jax.random.randint(jax.random.fold_in(stream_key, axis), (), 0, dims[axis]) for axis in range(len(dims))]
    drawn = drawn.at[tuple(spot)].set(smallest)
    longest = dims.index(max(dims))
    spot[longest] = (spot[longest] + 1) % dims[longest]
    return drawn.at[tuple(spot)].set(high)


def block_levels(key, dims, cuts, least, high):
    loudness, own = 1.0, jax.random.fold_in(key, 6)
    for dim, parts in cuts:
        draws = jnp.exp(jax.random.uniform(jax.random.fold_in(own, dim), (parts,), jnp.float32, least / len(cuts), high / len(cuts)))
        loudness = loudness * jnp.repeat(draws, dims[dim] // parts).reshape([-1 if axis == dim else 1 for axis in range(len(dims))])
    return loudness


def rank_bounds(number_of, skew):
    loads = [(1 << 20) // math.isqrt(standing ** skew) + 1 for standing in range(1, number_of + 1)]
    deviation = 1 + sum(loads) // (1 << 30)
    return np.cumsum(np.array([max(1, weight // deviation) for weight in loads]))


def ranked_ids(rng, extent, count, skew):
    table = rank_bounds(count, skew)
    lot = jax.random.randint(jax.random.fold_in(rng, 1), extent, 0, int(table[count - 1]))
    rank = jnp.searchsorted(jnp.asarray(table, jnp.int32), lot, side="right")
    return jax.random.permutation(jax.random.fold_in(rng, 2), count)[rank].astype(jnp.int32)


def split_up(count, total, most, skew):
    loads = [(1 << 20) // math.isqrt(standing ** skew) + 1 for standing in range(2, count + 1)]
    spare, counts = total - most - (count - 1), [1] * (count - 1)
    while spare > 0:
        free = [i for i in range(count - 1) if counts[i] < most]
        whole, remaining = sum([loads[i] for i in free]), spare
        for i in free:
            extra = min(most - counts[i], max(1, remaining * loads[i] // whole), spare)
            counts[i] = counts[i] + extra
            spare = spare - extra
    return np.array([most] + counts)


def ragged_sizes(key, count, total, reach, lean):
    if count == 2:
        one = jax.random.randint(key, (), max(1, total - reach), min(reach, total - 1) + 1)
        return jnp.stack([one, total - one])
    tallies = jnp.asarray(split_up(count, total, reach, lean), jnp.int32)
    couples = (count - 1) // 2
    source_of, taker = tallies[1:1 + 2 * couples:2], tallies[2:2 + 2 * couples:2]
    room = jnp.minimum(source_of - 1, reach - taker)
    shifted = jax.random.randint(jax.random.fold_in(key, 1), (couples,), 0, 1 << 20) % (room + 1)
    tallies = tallies.at[1:1 + 2 * couples:2].set(source_of - shifted).at[2:2 + 2 * couples:2].set(taker + shifted)
    return tallies[jax.random.permutation(jax.random.fold_in(key, 2), count)]


def gaussian(rng, dims, width, limit, pieces=(), kind=jnp.bfloat16):
    array = jax.random.normal(rng, dims, jnp.float32) * width
    if len(pieces) > 0:
        array = block_levels(rng, dims, pieces, -0.22, 0.18) * array
    return jnp.clip(array, min=-limit, max=limit).astype(kind)


def setup_inputs(seed: int = 0, part: int = 0) -> dict:
    key_list = jax.random.split(jax.random.key(seed), 11)
    part_splits = jax.random.split(jax.random.fold_in(key_list[10], part), 11)
    return {
        "queries": draw_queries(jax.random.fold_in(jax.random.fold_in(key_list[10], part), 71), part),
        "new_keys": draw_new_keys(jax.random.fold_in(jax.random.fold_in(key_list[10], part), 71), part),
        "new_values": gaussian(part_splits[2], (B, KV * HD), 2.0, 12.0, ((0, 16),)),
        "suffix_keys": gaussian(part_splits[3], (B, SUF, KV * HD), 3.0, 18.0, ((0, 16),)),
        "suffix_values": gaussian(part_splits[4], (B, SUF, KV * HD), 2.0, 12.0, ((0, 16),)),
        "suffix_lens": ragged_sizes(part_splits[5], B, B * SUF // 2, SUF, 2).astype(jnp.int32),
        "prefix_keys": gaussian(part_splits[6], (PAGES, PAGE, KV * HD), 2.0, 12.0, ((0, 16),)),
        "prefix_values": gaussian(part_splits[7], (PAGES, PAGE, KV * HD), 2.0, 12.0, ((0, 16),)),
        "page_table": draw_page_table(jax.random.fold_in(jax.random.fold_in(key_list[10], part), 71), part),
        "prefix_id": set_ends(ranked_ids(part_splits[9], (B,), NPREF, 2), jax.random.fold_in(part_splits[9], 3), 0, NPREF - 1).astype(jnp.int32),
    }


def reference(queries, new_keys, new_values, suffix_keys, suffix_values, suffix_lens, prefix_keys, prefix_values, page_table, prefix_id):
    group_size = H // KV
    softmax_scale = 1.0 / math.sqrt(HD)
    block_tokens = PAGES_DEV * PAGE
    page_ids = jnp.arange(PAGES, dtype=jnp.int32)
    page_hits = jnp.any(page_table[:, :, None] == page_ids[None, None, :], axis=1)
    prefix_of_page = lax.optimization_barrier(jnp.sum(page_hits.astype(jnp.int32) * jnp.arange(NPREF, dtype=jnp.int32)[:, None], axis=0))
    token_label = jnp.repeat(prefix_of_page, PAGE)
    pool_keys = prefix_keys.reshape(PAGES * PAGE, KV, HD).astype(jnp.float32)
    pool_values = prefix_values.reshape(N_SEQ, block_tokens, KV, HD).astype(jnp.float32)
    block_count = B // B_DEV
    slot_index = jnp.arange(SUF, dtype=jnp.int32)

    def one_block(inputs):
        block_queries, block_new_keys, block_new_values, block_suffix_keys, block_suffix_values, block_lens, block_ids = inputs
        query_head_count = block_queries.reshape(B_DEV, KV, group_size, HD).astype(jnp.float32)
        prefix_scores = jnp.einsum('bkgd,tkd->bkgt', query_head_count, pool_keys) * softmax_scale
        prefix_live = (block_ids[:, None] == token_label[None, :])[:, None, None, :]
        prefix_scores = jnp.where(prefix_live, prefix_scores, -1e+30)
        prefix_scores = prefix_scores.reshape(B_DEV, KV, group_size, N_SEQ, block_tokens)
        prefix_live = prefix_live.reshape(B_DEV, 1, 1, N_SEQ, block_tokens)
        block_peak = lax.optimization_barrier(jnp.max(prefix_scores, axis=4))
        block_weights = jnp.where(prefix_live, jnp.exp(prefix_scores - block_peak[..., None]), 0.0)
        block_mass = lax.optimization_barrier(jnp.sum(block_weights, axis=4))
        block_round = lax.optimization_barrier(block_weights.astype(jnp.bfloat16)).astype(jnp.float32)
        block_numer = jnp.einsum('bkgot,otkd->bkgod', block_round, pool_values)
        block_out = block_numer / block_mass[..., None]
        block_out = lax.optimization_barrier(block_out.astype(jnp.bfloat16)).astype(jnp.float32)
        block_lse = block_peak + jnp.log(block_mass)
        own_keys = block_suffix_keys.reshape(B_DEV, SUF, KV, HD).astype(jnp.float32)
        own_values = block_suffix_values.reshape(B_DEV, SUF, KV, HD).astype(jnp.float32)
        suffix_scores = jnp.einsum('bkgd,btkd->bkgt', query_head_count, own_keys) * softmax_scale
        suffix_live = (slot_index[None, :] < block_lens[:, None])[:, None, None, :]
        suffix_scores = jnp.where(suffix_live, suffix_scores, -1e+30)
        incoming_keys = block_new_keys.reshape(B_DEV, KV, HD).astype(jnp.float32)
        incoming_values = block_new_values.reshape(B_DEV, KV, HD).astype(jnp.float32)
        incoming_scores = jnp.einsum('iqnc,iqc->iqn', query_head_count, incoming_keys) * softmax_scale
        home_peak = jnp.maximum(lax.optimization_barrier(jnp.max(suffix_scores, axis=3)), incoming_scores)
        suffix_weights = jnp.where(suffix_live, jnp.exp(suffix_scores - home_peak[..., None]), 0.0)
        fresh_weights = jnp.exp(incoming_scores - home_peak)
        home_mass = lax.optimization_barrier(jnp.sum(suffix_weights, axis=3)) + fresh_weights
        suffix_round = lax.optimization_barrier(suffix_weights.astype(jnp.bfloat16)).astype(jnp.float32)
        incoming_rounded = lax.optimization_barrier(fresh_weights.astype(jnp.bfloat16)).astype(jnp.float32)
        resident_numerator = jnp.einsum('bkgt,btkd->bkgd', suffix_round, own_values)
        resident_numerator = resident_numerator + jnp.einsum('cqx,cqh->cqxh', incoming_rounded, incoming_values)
        home_out = resident_numerator / home_mass[..., None]
        home_lse = home_peak + jnp.log(home_mass)
        overall = jnp.maximum(lax.optimization_barrier(jnp.max(block_lse, axis=3)), home_lse)
        factor = jnp.exp(block_lse - overall[..., None])
        home_factor = jnp.exp(home_lse - overall)
        merged = lax.optimization_barrier(jnp.sum(factor[..., None] * block_out, axis=3)) + home_factor[..., None] * home_out
        divisor = lax.optimization_barrier(jnp.sum(factor, axis=3)) + home_factor
        result = merged / divisor[..., None]
        return result.reshape(B_DEV, H * HD).astype(jnp.bfloat16)
    stacked = (queries.reshape(block_count, B_DEV, H * HD), new_keys.reshape(block_count, B_DEV, KV * HD), new_values.reshape(block_count, B_DEV, KV * HD), suffix_keys.reshape(block_count, B_DEV, SUF, KV * HD), suffix_values.reshape(block_count, B_DEV, SUF, KV * HD), suffix_lens.reshape(block_count, B_DEV), prefix_id.reshape(block_count, B_DEV))
    outputs = lax.map(one_block, stacked)
    return outputs.reshape(B, H * HD)
```

```python
import functools
import math

import jax
import jax.numpy as jnp
from jax import lax
from jax.experimental import pallas as pl
from jax.experimental.pallas import tpu as pltpu
from jax.sharding import PartitionSpec as P

H = 32
KV = 8
HD = 128
NPREF = 2
G = H // KV
HALF = KV // 2
MASKED = -1e30
SCALE2 = math.log2(math.e) / math.sqrt(HD)
NT = (((1,), (1,)), ((), ()))
MESH = pl.DeviceIdType.MESH


def low_bit(m):
    return m & (-m)


def kernel(
    n, page,
    q_hbm, nk_ref, nv_ref, sk_hbm, sv_hbm, lens_ref, pk_hbm, pv_hbm, table_ref, pid_ref,
    out_ref,
    q_own, qs, sk, sv, pk, pv, vt, label, onehot, scores,
    part, lse, near, near_l, far, far_l, fin, fin_l, got, got_l, cols, cols_got,
    q_rows, nk_rows, nv_rows, home_o, home_l,
    in_sem, suf_sem, kv_send, kv_recv, ag_send, ag_recv,
    o_send, o_recv, l_send, l_recv, f_send, f_recv,
):
    rows = q_hbm.shape[0]
    slots = sk.shape[1]
    tokens = pk_hbm.shape[0]
    wide_cols = H * HD // 2
    kv_cols = KV * HD // 2
    lanes = 2 * rows * G
    chips = n // 2
    me = lax.axis_index("seq")
    core = me % 2
    chip = me // 2
    other = 1 - core

    def chip_xor(m):
        index = chip
        bit = 1
        while bit < chips:
            if m & bit:
                index = index + bit * (1 - 2 * ((chip // bit) % 2))
            bit *= 2
        return index

    def dev(m, c):
        return chip_xor(m) * 2 + c

    bits = [1 << i for i in range(chips.bit_length() - 1)]
    evens = [m for m in range(2, chips, 2)]

    def q_half(h):
        return pl.ds(pl.multiple_of(h * wide_cols, wide_cols), wide_cols)

    def kv_half(h):
        return pl.ds(pl.multiple_of(h * kv_cols, kv_cols), kv_cols)

    def token_half(h):
        return pl.ds(pl.multiple_of(h * tokens, tokens), tokens)

    def remote(src, dst, send, recv, where):
        return pltpu.make_async_remote_copy(
            src_ref=src, dst_ref=dst, send_sem=send, recv_sem=recv,
            device_id={"seq": where}, device_id_type=MESH,
        )

    q_copy = pltpu.make_async_copy(q_hbm, q_own, in_sem.at[0])
    q_mine = pltpu.make_async_copy(q_hbm.at[:, q_half(core)], qs.at[0, core], in_sem.at[1])
    k_mine = pltpu.make_async_copy(
        pk_hbm.at[:, kv_half(core)], pk.at[token_half(core)], in_sem.at[2])
    v_mine = pltpu.make_async_copy(
        pv_hbm.at[:, kv_half(core)], pv.at[token_half(core)], in_sem.at[3])
    q_copy.start()
    q_mine.start()

    def suffix_copies(b):
        return (
            pltpu.make_async_copy(sk_hbm.at[b], sk.at[b], suf_sem.at[0, b]),
            pltpu.make_async_copy(sv_hbm.at[b], sv.at[b], suf_sem.at[1, b]),
        )

    barrier = pltpu.get_barrier_semaphore()
    peers = [dev(0, other)]
    for b in bits:
        peers += [dev(b, 0), dev(b, 1)]
    peers += [dev(m, core) for m in evens if m & (m - 1)]
    for peer in peers:
        pl.semaphore_signal(barrier, inc=1, device_id={"seq": peer}, device_id_type=MESH)
    for b in range(rows // 2):
        for copy in suffix_copies(b):
            copy.start()
    k_mine.start()
    v_mine.start()
    for b in range(rows // 2, rows):
        for copy in suffix_copies(b):
            copy.start()
    pl.semaphore_wait(barrier, len(peers))
    q_copy.wait()

    def own_copy(b, h):
        return remote(
            q_own.at[:, h * wide_cols:(h + 1) * wide_cols], qs.at[b, core],
            ag_send.at[b, h], ag_recv.at[b, core], dev(b, h))

    def forward_copy(m, s):
        return remote(
            qs.at[m ^ low_bit(m), s], qs.at[m, s],
            ag_send.at[m, s], ag_recv.at[m, s], dev(low_bit(m), core))

    partner_q = remote(
        q_own.at[:, q_half(other)], qs.at[0, core],
        ag_send.at[0, 0], ag_recv.at[0, 0], dev(0, other))
    partner_kv = [
        remote(src.at[:, kv_half(other)], dst.at[token_half(core)],
               kv_send.at[i], kv_recv.at[i], dev(0, other))
        for i, (src, dst) in enumerate(((pk_hbm, pk), (pv_hbm, pv)))
    ]

    for b in reversed(bits):
        for h in range(2):
            own_copy(b, h).start()
    partner_q.start()
    for copy in partner_kv:
        copy.start()

    arrived = set([0])

    def arrive(m):
        if m in arrived:
            return
        arrived.add(m)
        arrive(m ^ low_bit(m))
        for s in range(2):
            if m & (m - 1):
                forward_copy(m, s).wait_recv()
            else:
                remote(
                    q_own.at[:, 0:wide_cols], qs.at[m, s],
                    ag_send.at[m, s], ag_recv.at[m, s], dev(m, core)).wait_recv()
            for bit in reversed(bits):
                if bit < low_bit(m):
                    forward_copy(m + bit, s).start()

    lse[...] = jnp.zeros(lse.shape, jnp.float32)

    for h in range(H):
        at = pl.ds(h, rows, stride=H)
        k = h // G
        q_rows[at, :] = q_own[:, h * HD:(h + 1) * HD].astype(jnp.float32)
        nk_rows[at, :] = nk_ref[:, k * HD:(k + 1) * HD].astype(jnp.float32)
        nv_rows[at, :] = nv_ref[:, k * HD:(k + 1) * HD].astype(jnp.float32)

    row_head = lax.broadcasted_iota(jnp.int32, (H, HD), 0) // G
    slot_iota = lax.broadcasted_iota(jnp.int32, (H, slots), 1)

    def suffix_one(b):
        at = pl.ds(pl.multiple_of(b * H, H), H)
        q = q_rows[at, :]
        wide = jnp.concatenate(
            [jnp.where(row_head == k, q, 0.0) for k in range(KV)], axis=1
        ).astype(jnp.bfloat16)
        s = lax.dot_general(wide, sk[b], NT, preferred_element_type=jnp.float32)
        s = jnp.where(slot_iota < lens_ref[b], s, MASKED)
        sn = jnp.sum(q * nk_rows[at, :], axis=1, keepdims=True)
        peak = jnp.maximum(jnp.max(s, axis=1, keepdims=True), sn)
        p = jnp.exp2((s - peak) * SCALE2)
        pn = jnp.exp2((sn - peak) * SCALE2)
        mass = jnp.sum(p, axis=1, keepdims=True) + pn
        o = jnp.dot(p.astype(jnp.bfloat16), sv[b], preferred_element_type=jnp.float32)
        own = pn * nv_rows[at, :]
        for k in range(KV):
            own = own + jnp.where(row_head == k, o[:, k * HD:(k + 1) * HD], 0.0)
        home_o[at, :] = own / mass
        home_l[at, :] = jnp.broadcast_to(peak * SCALE2 + jnp.log2(mass), (H, HD))

    def suffix(first, last):
        for b in range(first, last):
            for copy in suffix_copies(b):
                copy.wait()
        for b in range(first, last):
            suffix_one(b)

    def prepare_labels():
        seqs = n * rows
        diag = (lax.broadcasted_iota(jnp.int32, (seqs, seqs), 0)
                == lax.broadcasted_iota(jnp.int32, (seqs, seqs), 1))
        pid = jnp.sum(jnp.where(diag, pid_ref[...].astype(jnp.float32), 0.0), axis=1, keepdims=True)
        lane = lax.broadcasted_iota(jnp.int32, (seqs, HD), 1).astype(jnp.float32)
        onehot[...] = jnp.where(lane == pid, 1.0, 0.0).astype(jnp.bfloat16)
        pages = 2 * tokens // page
        entries = table_ref.shape[1]
        ids = chip * pages + lax.broadcasted_iota(jnp.int32, (pages, entries), 0)
        page_lane = lax.broadcasted_iota(jnp.int32, (pages, HD), 1)
        bar = jnp.zeros((pages, HD), jnp.float32)
        for p in range(NPREF):
            hit = jnp.max(
                jnp.where(table_ref[p:p + 1, :] == ids, 1.0, 0.0), axis=1, keepdims=True)
            bar = jnp.where(page_lane == p, (1.0 - hit) * MASKED, bar)
        token = lax.broadcasted_iota(jnp.int32, (2 * tokens, pages), 0)
        first = lax.broadcasted_iota(jnp.int32, (2 * tokens, pages), 1) * page
        spread = jnp.where((token >= first) & (token < first + page), 1.0, 0.0)
        label[...] = jnp.dot(
            spread.astype(jnp.bfloat16), bar.astype(jnp.bfloat16),
            preferred_element_type=jnp.float32).astype(jnp.bfloat16)

    def prepare_values():
        v_mine.wait()
        partner_kv[1].wait_recv()
        step = 256
        for k in range(HALF):
            for t in range(0, 2 * tokens, step):
                vt[k, :HD, t:t + step] = pv[t:t + step, k * HD:(k + 1) * HD].T
            vt[k, HD:, :] = jnp.ones((vt.shape[1] - HD, 2 * tokens), jnp.bfloat16)

    def compute(blocks, j):
        parts = [(m, s) for m in blocks for s in range(2)]
        code = jnp.concatenate(
            [onehot[pl.ds(pl.multiple_of(dev(m, s) * rows, rows), rows), :]
             for m, s in parts for g in range(G)], axis=0)
        for i in range(HALF // 2):
            k = j * (HALF // 2) + i
            buf = scores.at[i]
            q = jnp.concatenate(
                [qs[m, s, :, (k * G + g) * HD:(k * G + g + 1) * HD]
                 for m, s in parts for g in range(G)], axis=0)
            qx = jnp.concatenate([q, code], axis=1)
            step = 512
            peak = None
            for t in range(0, 2 * tokens, step):
                kx = jnp.concatenate(
                    [pk[t:t + step, k * HD:(k + 1) * HD], label[t:t + step, :]], axis=1)
                s = lax.dot_general(kx, qx, NT, preferred_element_type=jnp.float32)
                buf[t:t + step, :] = s
                top = jnp.max(s, axis=0, keepdims=True)
                peak = top if peak is None else jnp.maximum(peak, top)
            o = None
            for t in range(0, 2 * tokens, step):
                p = jnp.exp2((buf[t:t + step, :] - peak) * SCALE2).astype(jnp.bfloat16)
                d = jnp.dot(vt[k, :, t:t + step], p, preferred_element_type=jnp.float32)
                o = d if o is None else o + d
            mass = o[HD:HD + 1, :]
            res = (o[:HD, :] * (1.0 / mass)).astype(jnp.bfloat16)
            level = peak * SCALE2 + jnp.log2(mass)
            for x, m in enumerate(blocks):
                part[m, j, i * HD:(i + 1) * HD, :] = res[:, x * lanes:(x + 1) * lanes]
                lse[m, j, i:i + 1, :] = level[:, x * lanes:(x + 1) * lanes]

    def near_copies(m, j):
        return [
            remote(part.at[m, j], near.at[m, j], o_send.at[m, j], o_recv.at[m, j], dev(1, core)),
            remote(lse.at[m, j], near_l.at[m, j], l_send.at[m, j], l_recv.at[m, j], dev(1, core)),
        ]

    def far_copies(m, j):
        return [
            remote(part.at[m, j], far.at[m, j], o_send.at[m, j], o_recv.at[m, j], dev(m, core)),
            remote(lse.at[m, j], far_l.at[m, j], l_send.at[m, j], l_recv.at[m, j], dev(m, core)),
        ]

    def send(copies):
        for copy in copies:
            copy.start()

    def merge(m, j, copies, src, src_l):
        for copy in copies:
            copy.wait_recv()
        for i in range(HALF // 2):
            la, lb = src_l[j, i:i + 1, :], lse[m, j, i:i + 1, :]
            w = 1.0 / (1.0 + jnp.exp2(lb - la))
            lse[m, j, i:i + 1, :] = jnp.maximum(la, lb) + jnp.log2(1.0 + jnp.exp2(-jnp.abs(la - lb)))
            at = slice(i * HD, (i + 1) * HD)
            a = src[j, at, :].astype(jnp.float32)
            b = part[m, j, at, :].astype(jnp.float32)
            part[m, j, at, :] = (b + (a - b) * w).astype(jnp.bfloat16)

    def merge_near(m, j):
        merge(m, j, near_copies(m + 1, j), near.at[m + 1], near_l.at[m + 1])

    def merge_far(m, j):
        merge(0, j, far_copies(m, j), far.at[m], far_l.at[m])

    def settle(m, j):
        merge_near(m, j)
        send(far_copies(m, j))

    quarter = max(1, rows // 4)
    cuts = [min(rows, quarter * i) for i in range(5)]
    arrive_after = {0: [], 1: [], 2: [], 3: []}
    by_count = sorted(evens, key=lambda m: (bin(m).count("1"), -m))
    for i, m in enumerate(by_count):
        arrive_after[min(3, 1 + i)].append(m)
    prepare_labels()
    for i in range(4):
        suffix(cuts[i], cuts[i + 1])
        for m in arrive_after[i]:
            arrive(m)
    k_mine.wait()
    partner_kv[0].wait_recv()
    q_mine.wait()
    remote(q_own.at[:, 0:wide_cols], qs.at[0, other],
           ag_send.at[0, 0], ag_recv.at[0, 0], dev(0, other)).wait_recv()
    prepare_values()

    order = by_count[::-1] if False else sorted(evens, key=lambda m: (bin(m).count("1"), m))
    waiting = []
    for m in order + [0]:
        arrive(m)
        arrive(m + 1)
        for j in range(2):
            compute([m, m + 1], j)
            send(near_copies(m + 1, j))
            for w in waiting:
                settle(w, j)
        waiting = [m] if m else []
    for j in range(2):
        merge_near(0, j)
    for m in order:
        for j in range(2):
            merge_far(m, j)

    def column(src):
        return jnp.concatenate([src] * (HD // src.shape[0]), axis=0).T

    for j in range(2):
        for i in range(HALF // 2):
            k = j * (HALF // 2) + i
            fin[k] = part[0, j, i * HD:(i + 1) * HD, :].astype(jnp.float32).T.astype(jnp.bfloat16)
    mine = rows * G
    give = remote(
        fin.at[:, pl.ds(pl.multiple_of(other * mine, mine), mine), :], got,
        f_send.at[0], f_recv.at[0], dev(0, other))
    give_l = remote(lse.at[0], got_l, f_send.at[1], f_recv.at[1], dev(0, other))
    give.start()
    give_l.start()

    def finish(half, levels, value):
        for k in range(HALF):
            j, i = k // (HALF // 2), k % (HALF // 2)
            for g in range(G):
                head = half * (HALF * G) + k * G + g
                level = levels[j, pl.ds(pl.multiple_of(core * mine + g * rows, rows), rows), i:i + 1]
                x = value(k, g).astype(jnp.float32)
                at = pl.ds(head, rows, stride=H)
                home = home_o[at, :]
                w = 1.0 / (1.0 + jnp.exp2(level - home_l[at, :]))
                out_ref[:, pl.ds(pl.multiple_of(head * HD, HD), HD)] = (
                    x + (home - x) * w).astype(jnp.bfloat16)

    for j in range(2):
        cols[j] = column(lse[0, j])
    finish(core, cols, lambda k, g: fin[
        k, pl.ds(pl.multiple_of(core * mine + g * rows, rows), rows), :])
    give.wait_recv()
    give_l.wait_recv()
    for j in range(2):
        cols_got[j] = column(got_l[j])
    finish(other, cols_got, lambda k, g: got[k, g * rows:(g + 1) * rows, :])

    for b in bits:
        for h in range(2):
            own_copy(b, h).wait_send()
    for m in range(1, chips):
        if m & (m - 1):
            for s in range(2):
                forward_copy(m, s).wait_send()
    partner_q.wait_send()
    for copy in partner_kv:
        copy.wait_send()
    for m in range(1, chips):
        for j in range(2):
            for copy in (near_copies(m, j) if m % 2 else far_copies(m, j)):
                copy.wait_send()
    give.wait_send()
    give_l.wait_send()


def local(
    queries, new_keys, new_values, suffix_keys, suffix_values, suffix_lens,
    prefix_keys, prefix_values, page_table, prefix_id,
):
    n = lax.axis_size("seq")
    chips = n // 2
    rows = queries.shape[0]
    slots = suffix_keys.shape[1]
    pages, page, width = prefix_keys.shape
    tokens = pages * page
    vmem = pl.BlockSpec(memory_space=pltpu.VMEM)
    hbm = pl.BlockSpec(memory_space=pl.ANY)
    smem = pl.BlockSpec(memory_space=pltpu.SMEM)
    bf16, f32 = jnp.bfloat16, jnp.float32
    dma = pltpu.SemaphoreType.DMA
    lanes = 2 * rows * G
    deep = HALF // 2 * HD
    return pl.pallas_call(
        functools.partial(kernel, n, page),
        out_shape=jax.ShapeDtypeStruct((rows, H * HD), bf16),
        in_specs=[hbm, vmem, vmem, hbm, hbm, smem, hbm, hbm, vmem, vmem],
        out_specs=vmem,
        scratch_shapes=[
            pltpu.VMEM((rows, H * HD), bf16),
            pltpu.VMEM((chips, 2, rows, H * HD // 2), bf16),
            pltpu.VMEM((rows, slots, width), bf16),
            pltpu.VMEM((rows, slots, width), bf16),
            pltpu.VMEM((2 * tokens, width // 2), bf16),
            pltpu.VMEM((2 * tokens, width // 2), bf16),
            pltpu.VMEM((HALF, HD + 16, 2 * tokens), bf16),
            pltpu.VMEM((2 * tokens, HD), bf16),
            pltpu.VMEM((n * rows, HD), bf16),
            pltpu.VMEM((HALF // 2, 2 * tokens, 2 * lanes), f32),
            pltpu.VMEM((chips, 2, deep, lanes), bf16),
            pltpu.VMEM((chips, 2, 8, lanes), f32),
            pltpu.VMEM((chips, 2, deep, lanes), bf16),
            pltpu.VMEM((chips, 2, 8, lanes), f32),
            pltpu.VMEM((chips, 2, deep, lanes), bf16),
            pltpu.VMEM((chips, 2, 8, lanes), f32),
            pltpu.VMEM((HALF, lanes, HD), bf16),
            pltpu.VMEM((2, 8, lanes), f32),
            pltpu.VMEM((HALF, rows * G, HD), bf16),
            pltpu.VMEM((2, 8, lanes), f32),
            pltpu.VMEM((2, lanes, HD), f32),
            pltpu.VMEM((2, lanes, HD), f32),
            pltpu.VMEM((rows * H, HD), f32),
            pltpu.VMEM((rows * H, HD), f32),
            pltpu.VMEM((rows * H, HD), f32),
            pltpu.VMEM((rows * H, HD), f32),
            pltpu.VMEM((rows * H, HD), f32),
            dma((4,)),
            dma((2, rows)),
            dma((2,)), dma((2,)),
            dma((chips, 2)), dma((chips, 2)),
            dma((chips, 2)), dma((chips, 2)), dma((chips, 2)), dma((chips, 2)),
            dma((2,)), dma((2,)),
        ],
        compiler_params=pltpu.CompilerParams(
            collective_id=0, has_side_effects=True, vmem_limit_bytes=64 * 1024 * 1024 - 65536,
        ),
        name="step",
    )(
        queries, new_keys, new_values, suffix_keys, suffix_values, suffix_lens,
        prefix_keys.reshape(tokens, width), prefix_values.reshape(tokens, width),
        page_table, prefix_id.reshape(1, n * rows),
    )


def solution(mesh):
    return jax.shard_map(
        local,
        mesh=mesh,
        in_specs=(
            P(("grp", "seq"), None),
            P(("grp", "seq"), None),
            P(("grp", "seq"), None),
            P(("grp", "seq"), None, None),
            P(("grp", "seq"), None, None),
            P(("grp", "seq")),
            P(("grp", "seq"), None, None),
            P(("grp", "seq"), None, None),
            P("grp", None),
            P("grp"),
        ),
        out_specs=P(("grp", "seq"), None),
        check_vma=False,
    )
```

```python
import functools
import math

import jax
import jax.numpy as jnp
from jax import lax
from jax.experimental import pallas as pl
from jax.experimental.pallas import tpu as pltpu
from jax.sharding import PartitionSpec as P

H = 32
KV = 8
HD = 128
NPREF = 2
G = H // KV
HALF = KV // 2
MASKED = -1e30
SCALE2 = math.log2(math.e) / math.sqrt(HD)
NT = (((1,), (1,)), ((), ()))
MESH = pl.DeviceIdType.MESH


def low_bit(m):
    return m & (-m)


def kernel(
    n, page,
    q_hbm, nk_hbm, nv_hbm, sk_hbm, sv_hbm, lens_ref, pk_hbm, pv_hbm, table_hbm, pid_hbm,
    out_ref,
    nk_ref, nv_ref, table_ref, pid_ref,
    q_own, qs, sk, sv, pk, pv, vt, label, onehot, scores,
    part, lse, near, near_l, fin, got, got_l, cols, cols_got,
    q_rows, nk_rows, nv_rows, home_o, home_l, home_m, weights,
    in_sem, fence, suf_sem, kv_send, kv_recv, ag_send, ag_recv,
    o_send, o_recv, l_send, l_recv, f_send, f_recv,
):
    rows = q_hbm.shape[0]
    slots = sk.shape[1]
    tokens = pk_hbm.shape[0]
    wide_cols = H * HD // 2
    kv_cols = KV * HD // 2
    lanes = 2 * rows * G
    chips = n // 2
    me = lax.axis_index("seq")
    core = me % 2
    chip = me // 2
    other = 1 - core

    def chip_xor(m):
        index = chip
        bit = 1
        while bit < chips:
            if m & bit:
                index = index + bit * (1 - 2 * ((chip // bit) % 2))
            bit *= 2
        return index

    def dev(m, c):
        return chip_xor(m) * 2 + c

    bits = [1 << i for i in range(chips.bit_length() - 1)]
    evens = [m for m in range(2, chips, 2)]
    top_bit = bits[-1]
    middle = bits[1:-1]
    q_paths = (bits[::-1], [top_bit, 1] + middle[::-1])
    o_paths = (None, None) * (HALF // 2)

    def q_hop(m, s):
        return [b for b in q_paths[s] if m & b][-1]

    def o_hop(m, j):
        if o_paths[j] is None:
            return 1 if m % 2 else m
        return [b for b in o_paths[j] if m & b][0]

    def o_children(m, j):
        return [x for x in range(1, chips) if x ^ o_hop(x, j) == m]


    def q_half(h):
        return pl.ds(pl.multiple_of(h * wide_cols, wide_cols), wide_cols)

    def kv_half(h):
        return pl.ds(pl.multiple_of(h * kv_cols, kv_cols), kv_cols)

    def token_half(h):
        return pl.ds(pl.multiple_of(h * tokens, tokens), tokens)

    def remote(src, dst, send, recv, where):
        return pltpu.make_async_remote_copy(
            src_ref=src, dst_ref=dst, send_sem=send, recv_sem=recv,
            device_id={"seq": where}, device_id_type=MESH,
        )

    q_copy = pltpu.make_async_copy(q_hbm, q_own, in_sem.at[0])
    q_mine = pltpu.make_async_copy(q_hbm.at[:, q_half(core)], qs.at[0, core], in_sem.at[1])
    k_mine = pltpu.make_async_copy(
        pk_hbm.at[:, kv_half(core)], pk.at[token_half(core)], in_sem.at[2])
    v_mine = pltpu.make_async_copy(
        pv_hbm.at[:, kv_half(core)], pv.at[token_half(core)], in_sem.at[3])
    small = [
        pltpu.make_async_copy(src, dst, in_sem.at[4 + i])
        for i, (src, dst) in enumerate((
            (nk_hbm, nk_ref), (nv_hbm, nv_ref), (table_hbm, table_ref), (pid_hbm, pid_ref)))
    ]
    q_copy.start()
    q_mine.start()
    for copy in small:
        copy.start()

    def suffix_copies(b):
        return (
            pltpu.make_async_copy(sk_hbm.at[b], sk.at[b], suf_sem.at[0, b]),
            pltpu.make_async_copy(sv_hbm.at[b], sv.at[b], suf_sem.at[1, b]),
        )

    barrier = pltpu.get_barrier_semaphore()
    peers = [dev(0, other)]
    for b in bits:
        peers += [dev(b, 0), dev(b, 1)]
    peers += [dev(m, core) for m in evens if m & (m - 1)]
    for peer in peers:
        pl.semaphore_signal(barrier, inc=1, device_id={"seq": peer}, device_id_type=MESH)
    for b in range(rows // 2):
        for copy in suffix_copies(b):
            copy.start()
    k_mine.start()
    v_mine.start()
    for b in range(rows // 2, rows):
        for copy in suffix_copies(b):
            copy.start()
    pl.semaphore_wait(barrier, len(peers))
    q_copy.wait()

    def own_copy(b, h):
        return remote(
            q_own.at[:, h * wide_cols:(h + 1) * wide_cols], qs.at[b, core],
            ag_send.at[b, h], ag_recv.at[b, core], dev(b, h))

    def forward_copy(m, s):
        hop = q_hop(m, s)
        return remote(
            qs.at[m ^ hop, s], qs.at[m, s], ag_send.at[m, s], ag_recv.at[m, s], dev(hop, core))

    partner_q = remote(
        q_own.at[:, q_half(other)], qs.at[0, core],
        ag_send.at[0, 0], ag_recv.at[0, 0], dev(0, other))
    partner_kv = [
        remote(src.at[:, kv_half(other)], dst.at[token_half(core)],
               kv_send.at[i], kv_recv.at[i], dev(0, other))
        for i, (src, dst) in enumerate(((pk_hbm, pk), (pv_hbm, pv)))
    ]

    for b in bits:
        for h in range(2):
            own_copy(b, h).start()
    partner_q.start()
    for copy in partner_kv:
        copy.start()

    arrived = set([(0, 0), (0, 1)])

    def pull(m, s):
        if (m, s) in arrived:
            return
        arrived.add((m, s))
        hop = q_hop(m, s)
        pull(m ^ hop, s)
        if m == hop:
            remote(
                q_own.at[:, 0:wide_cols], qs.at[m, s],
                ag_send.at[m, s], ag_recv.at[m, s], dev(m, core)).wait_recv()
        else:
            forward_copy(m, s).wait_recv()
        for b in reversed(q_paths[s][q_paths[s].index(hop) + 1:]):
            forward_copy(m | b, s).start()

    def arrive(m):
        for s in range(2):
            pull(m, s)

    for copy in small:
        copy.wait()

    for h in range(H):
        at = pl.ds(h, rows, stride=H)
        k = h // G
        q_rows[at, :] = q_own[:, h * HD:(h + 1) * HD].astype(jnp.float32)
        nk_rows[at, :] = nk_ref[:, k * HD:(k + 1) * HD].astype(jnp.float32)
        nv_rows[at, :] = nv_ref[:, k * HD:(k + 1) * HD].astype(jnp.float32)

    row_head = lax.broadcasted_iota(jnp.int32, (H, HD), 0) // G
    slot_iota = lax.broadcasted_iota(jnp.int32, (H, slots), 1)

    def suffix_scores(b):
        at = slice(b * H, (b + 1) * H)
        q = q_rows[at, :]
        wide = jnp.concatenate(
            [jnp.where(row_head == k, q, 0.0) for k in range(KV)], axis=1
        ).astype(jnp.bfloat16)
        s = lax.dot_general(wide, sk[b], NT, preferred_element_type=jnp.float32)
        s = jnp.where(slot_iota < lens_ref[b], s, MASKED)
        sn = jnp.sum(q * nk_rows[at, :], axis=1, keepdims=True)
        peak = jnp.maximum(jnp.max(s, axis=1, keepdims=True), sn)
        p = jnp.exp2((s - peak) * SCALE2)
        pn = jnp.exp2((sn - peak) * SCALE2)
        mass = jnp.sum(p, axis=1, keepdims=True) + pn
        weights[at, :] = p.astype(jnp.bfloat16)
        home_l[at, :] = jnp.broadcast_to(peak * SCALE2 + jnp.log2(mass), (H, HD))
        home_m[at, :] = jnp.broadcast_to(1.0 / mass, (H, HD))
        home_o[at, :] = pn * nv_rows[at, :]

    def suffix_outputs(b):
        at = slice(b * H, (b + 1) * H)
        o = jnp.dot(weights[at, :], sv[b], preferred_element_type=jnp.float32)
        own = home_o[at, :]
        for k in range(KV):
            own = own + jnp.where(row_head == k, o[:, k * HD:(k + 1) * HD], 0.0)
        home_o[at, :] = own * home_m[at, :]

    def suffix(first, last):
        for b in range(first, last):
            suffix_copies(b)[0].wait()
        for b in range(first, last):
            suffix_scores(b)
        for b in range(first, last):
            suffix_copies(b)[1].wait()
        for b in range(first, last):
            suffix_outputs(b)

    def prepare_labels():
        seqs = n * rows
        diag = (lax.broadcasted_iota(jnp.int32, (seqs, seqs), 0)
                == lax.broadcasted_iota(jnp.int32, (seqs, seqs), 1))
        pid = jnp.sum(jnp.where(diag, pid_ref[...].astype(jnp.float32), 0.0), axis=1, keepdims=True)
        lane = lax.broadcasted_iota(jnp.int32, (seqs, HD), 1).astype(jnp.float32)
        onehot[...] = jnp.where(lane == pid, 1.0, 0.0).astype(jnp.bfloat16)
        pages = 2 * tokens // page
        entries = table_ref.shape[1]
        ids = chip * pages + lax.broadcasted_iota(jnp.int32, (pages, entries), 0)
        page_lane = lax.broadcasted_iota(jnp.int32, (pages, HD), 1)
        bar = jnp.zeros((pages, HD), jnp.float32)
        for p in range(NPREF):
            hit = jnp.max(
                jnp.where(table_ref[p:p + 1, :] == ids, 1.0, 0.0), axis=1, keepdims=True)
            bar = jnp.where(page_lane == p, (1.0 - hit) * MASKED, bar)
        token = lax.broadcasted_iota(jnp.int32, (2 * tokens, pages), 0)
        first = lax.broadcasted_iota(jnp.int32, (2 * tokens, pages), 1) * page
        spread = jnp.where((token >= first) & (token < first + page), 1.0, 0.0)
        label[...] = jnp.dot(
            spread.astype(jnp.bfloat16), bar.astype(jnp.bfloat16),
            preferred_element_type=jnp.float32).astype(jnp.bfloat16)

    def prepare_values():
        v_mine.wait()
        partner_kv[1].wait_recv()
        for k in range(HALF):
            for t in starts:
                vt[k, :HD, t:t + step] = pv[t:t + step, k * HD:(k + 1) * HD].T
            vt[k, HD:, :] = jnp.ones((vt.shape[1] - HD, 2 * tokens), jnp.bfloat16)

    step = 256
    starts = range(0, 2 * tokens, step)

    def query_side(item):
        m, k = item
        parts = [(x, s) for x in (m, m + 1) for s in range(2)]
        code = jnp.concatenate(
            [onehot[pl.ds(pl.multiple_of(dev(x, s) * rows, rows), rows), :]
             for x, s in parts for g in range(G)], axis=0)
        q = jnp.concatenate(
            [qs[x, s, :, (k * G + g) * HD:(k * G + g + 1) * HD]
             for x, s in parts for g in range(G)], axis=0)
        return jnp.concatenate([q, code], axis=1)

    def advance(current, peak, following, slot):
        qx = None if following is None else query_side(following)
        top, o = None, None
        for t in starts:
            at = slice(t, t + step)
            if following is not None:
                k = following[1]
                kx = jnp.concatenate([pk[at, k * HD:(k + 1) * HD], label[at, :]], axis=1)
                s = lax.dot_general(kx, qx, NT, preferred_element_type=jnp.float32)
                scores[1 - slot, at, :] = s
                high = jnp.max(s, axis=0, keepdims=True)
                top = high if top is None else jnp.maximum(top, high)
            if current is not None:
                p = jnp.exp2((scores[slot, at, :] - peak) * SCALE2).astype(jnp.bfloat16)
                d = jnp.dot(vt[current[1], :, at], p, preferred_element_type=jnp.float32)
                o = d if o is None else o + d
        if current is not None:
            m, k = current
            mass = o[HD:HD + 1, :]
            res = (o[:HD, :] * (1.0 / mass)).astype(jnp.bfloat16)
            level = peak * SCALE2 + jnp.log2(mass)
            for x in range(2):
                part[m + x, k] = res[:, x * lanes:(x + 1) * lanes]
                lse[m + x, k] = level[:, x * lanes:(x + 1) * lanes]
        return top

    def part_copies(m, j):
        where = dev(o_hop(m, j), core)
        return [
            remote(part.at[m, j], near.at[m, j], o_send.at[m, j], o_recv.at[m, j], where),
            remote(lse.at[m, j], near_l.at[m, j], l_send.at[m, j], l_recv.at[m, j], where),
        ]

    def merge(m, child, j):
        for copy in part_copies(child, j):
            copy.wait_recv()
        la, lb = near_l[child, j], lse[m, j]
        w = 1.0 / (1.0 + jnp.exp2(lb - la))
        lse[m, j] = jnp.maximum(la, lb) + jnp.log2(1.0 + jnp.exp2(-jnp.abs(la - lb)))
        a = near[child, j].astype(jnp.float32)
        b = part[m, j].astype(jnp.float32)
        part[m, j] = (b + (a - b) * w).astype(jnp.bfloat16)

    def settle(m, j):
        for child in o_children(m, j):
            merge(m, child, j)
        if m:
            for copy in part_copies(m, j):
                copy.start()

    def split():
        pl.semaphore_signal(fence, 1)
        pl.semaphore_wait(fence, 1)

    ready, sent = set(), {}
    clock = [0]

    def depth(node):
        m, j = node
        return 0 if m == 0 else 1 + depth((m ^ o_hop(m, j), j))

    def progress(last):
        lag = 1 if last else 5
        for node in sorted(ready, key=lambda x: (-depth(x), -x[0], x[1])):
            if node[0] == 0 or (node[0] in (1,) and not last):
                continue
            kids = [(c, node[1]) for c in o_children(*node)]
            if all(kid in sent and sent[kid] + lag <= clock[0] for kid in kids):
                settle(*node)
                ready.remove(node)
                sent[node] = clock[0]

    quarter = max(1, rows // 4)
    batches = list(range(0, rows, quarter))

    def fill(count):
        for _ in range(count):
            if batches:
                b = batches.pop(0)
                suffix(b, b + quarter)
                clock[0] += 2

    groups = [0] + evens
    prepare_labels()
    fill(1)
    arrive(groups[1])
    k_mine.wait()
    partner_kv[0].wait_recv()
    q_mine.wait()
    remote(q_own.at[:, 0:wide_cols], qs.at[0, other],
           ag_send.at[0, 0], ag_recv.at[0, 0], dev(0, other)).wait_recv()
    prepare_values()
    for x, m in enumerate(groups):
        if x == len(groups) - 1:
            fill(0)
        arrive(m)
        arrive(m + 1)
        peak = advance(None, None, (m, 0), 1)
        split()
        for k in range(HALF):
            peak = advance((m, k), peak, (m, k + 1) if k + 1 < HALF else None, k % 2)
            split()
            ready |= {(m, k), (m + 1, k)}
            progress(False)
            clock[0] += 1
            if k == 1 and x + 2 < len(groups):
                arrive(groups[x + 2])
    while batches:
        fill(1)
        progress(False)
    while len(sent) < HALF * (chips - 1):
        progress(True)
        clock[0] += 1
    for j in range(HALF):
        settle(0, j)
        fin[j] = part[0, j].astype(jnp.float32).T.astype(jnp.bfloat16)

    def column(src):
        levels = jnp.concatenate([src[k] for k in range(HALF)], axis=0)
        return jnp.concatenate([levels] * (HD // HALF), axis=0).T

    mine = rows * G
    give = remote(
        fin.at[:, pl.ds(pl.multiple_of(other * mine, mine), mine), :], got,
        f_send.at[0], f_recv.at[0], dev(0, other))
    give_l = remote(lse.at[0], got_l, f_send.at[1], f_recv.at[1], dev(0, other))
    give.start()
    give_l.start()

    def finish(half, levels, value):
        for k in range(HALF):
            j, i = k // (HALF // 2), k % (HALF // 2)
            for g in range(G):
                head = half * (HALF * G) + k * G + g
                level = levels[pl.ds(pl.multiple_of(core * mine + g * rows, rows), rows), k:k + 1]
                x = value(k, g).astype(jnp.float32)
                at = pl.ds(head, rows, stride=H)
                home = home_o[at, :]
                w = 1.0 / (1.0 + jnp.exp2(level - home_l[at, :]))
                out_ref[:, pl.ds(pl.multiple_of(head * HD, HD), HD)] = (
                    x + (home - x) * w).astype(jnp.bfloat16)

    cols[...] = column(lse.at[0])
    finish(core, cols, lambda k, g: fin[
        k, pl.ds(pl.multiple_of(core * mine + g * rows, rows), rows), :])
    give.wait_recv()
    give_l.wait_recv()
    cols_got[...] = column(got_l)
    finish(other, cols_got, lambda k, g: got[k, g * rows:(g + 1) * rows, :])

    for b in bits:
        for h in range(2):
            own_copy(b, h).wait_send()
    for m in range(1, chips):
        if m & (m - 1):
            for s in range(2):
                forward_copy(m, s).wait_send()
    partner_q.wait_send()
    for copy in partner_kv:
        copy.wait_send()
    for m in range(1, chips):
        for j in range(HALF):
            for copy in part_copies(m, j):
                copy.wait_send()
    give.wait_send()
    give_l.wait_send()


def local(
    queries, new_keys, new_values, suffix_keys, suffix_values, suffix_lens,
    prefix_keys, prefix_values, page_table, prefix_id,
):
    n = lax.axis_size("seq")
    chips = n // 2
    rows = queries.shape[0]
    slots = suffix_keys.shape[1]
    pages, page, width = prefix_keys.shape
    tokens = pages * page
    vmem = pl.BlockSpec(memory_space=pltpu.VMEM)
    hbm = pl.BlockSpec(memory_space=pl.ANY)
    smem = pl.BlockSpec(memory_space=pltpu.SMEM)
    bf16, f32 = jnp.bfloat16, jnp.float32
    dma = pltpu.SemaphoreType.DMA
    lanes = 2 * rows * G
    return pl.pallas_call(
        functools.partial(kernel, n, page),
        out_shape=jax.ShapeDtypeStruct((rows, H * HD), bf16),
        in_specs=[hbm, hbm, hbm, hbm, hbm, smem, hbm, hbm, hbm, hbm],
        out_specs=vmem,
        scratch_shapes=[
            pltpu.VMEM((rows, width), bf16),
            pltpu.VMEM((rows, width), bf16),
            pltpu.VMEM(page_table.shape, jnp.int32),
            pltpu.VMEM((1, n * rows), jnp.int32),
            pltpu.VMEM((rows, H * HD), bf16),
            pltpu.VMEM((chips, 2, rows, H * HD // 2), bf16),
            pltpu.VMEM((rows, slots, width), bf16),
            pltpu.VMEM((rows, slots, width), bf16),
            pltpu.VMEM((2 * tokens, width // 2), bf16),
            pltpu.VMEM((2 * tokens, width // 2), bf16),
            pltpu.VMEM((HALF, HD + 16, 2 * tokens), bf16),
            pltpu.VMEM((2 * tokens, HD), bf16),
            pltpu.VMEM((n * rows, HD), bf16),
            pltpu.VMEM((2, 2 * tokens, 2 * lanes), f32),
            pltpu.VMEM((chips, HALF, HD, lanes), bf16),
            pltpu.VMEM((chips, HALF, 1, lanes), f32),
            pltpu.VMEM((chips, HALF, HD, lanes), bf16),
            pltpu.VMEM((chips, HALF, 1, lanes), f32),
            pltpu.VMEM((HALF, lanes, HD), bf16),
            pltpu.VMEM((HALF, rows * G, HD), bf16),
            pltpu.VMEM((HALF, 1, lanes), f32),
            pltpu.VMEM((lanes, HD), f32),
            pltpu.VMEM((lanes, HD), f32),
            pltpu.VMEM((rows * H, HD), f32),
            pltpu.VMEM((rows * H, HD), f32),
            pltpu.VMEM((rows * H, HD), f32),
            pltpu.VMEM((rows * H, HD), f32),
            pltpu.VMEM((rows * H, HD), f32),
            pltpu.VMEM((rows * H, HD), f32),
            pltpu.VMEM((rows * H, slots), bf16),
            dma((8,)),
            pltpu.SemaphoreType.REGULAR,
            dma((2, rows)),
            dma((2,)), dma((2,)),
            dma((chips, 2)), dma((chips, 2)),
            dma((chips, HALF)), dma((chips, HALF)), dma((chips, HALF)), dma((chips, HALF)),
            dma((2,)), dma((2,)),
        ],
        compiler_params=pltpu.CompilerParams(
            collective_id=0, has_side_effects=True, vmem_limit_bytes=64 * 1024 * 1024 - 65536,
        ),
        name="step",
    )(
        queries, new_keys, new_values, suffix_keys, suffix_values, suffix_lens,
        prefix_keys.reshape(tokens, width), prefix_values.reshape(tokens, width),
        page_table, prefix_id.reshape(1, n * rows),
    )


def solution(mesh):
    return jax.shard_map(
        local,
        mesh=mesh,
        in_specs=(
            P(("grp", "seq"), None),
            P(("grp", "seq"), None),
            P(("grp", "seq"), None),
            P(("grp", "seq"), None, None),
            P(("grp", "seq"), None, None),
            P(("grp", "seq")),
            P(("grp", "seq"), None, None),
            P(("grp", "seq"), None, None),
            P("grp", None),
            P("grp"),
        ),
        out_specs=P(("grp", "seq"), None),
        check_vma=False,
    )
```

```python
import functools
import math

import jax
import jax.numpy as jnp
from jax import lax
from jax.experimental import pallas as pl
from jax.experimental.pallas import tpu as pltpu
from jax.sharding import PartitionSpec as P

H = 32
KV = 8
HD = 128
NPREF = 2
G = H // KV
HALF = KV // 2
MASKED = -1e30
SCALE2 = math.log2(math.e) / math.sqrt(HD)
NT = (((1,), (1,)), ((), ()))
MESH = pl.DeviceIdType.MESH


def low_bit(m):
    return m & (-m)


def kernel(
    n, page,
    q_hbm, nk_hbm, nv_hbm, sk_hbm, sv_hbm, lens_ref, pk_hbm, pv_hbm, table_hbm, pid_hbm,
    out_ref,
    nk_ref, nv_ref, table_ref, pid_ref,
    q_own, qs, sk, sv, pk, pv, vt, label, onehot, scores,
    part, lse, near, near_l, fin, got, got_l, cols, cols_got,
    q_rows, nk_rows, nv_rows, home_o, home_l, home_m, weights,
    in_sem, fence, suf_sem, kv_send, kv_recv, ag_send, ag_recv,
    o_send, o_recv, l_send, l_recv, f_send, f_recv,
):
    rows = q_hbm.shape[0]
    slots = sk.shape[1]
    tokens = pk_hbm.shape[0]
    wide_cols = H * HD // 2
    kv_cols = KV * HD // 2
    lanes = 2 * rows * G
    chips = n // 2
    me = lax.axis_index("seq")
    core = me % 2
    chip = me // 2
    other = 1 - core

    def chip_xor(m):
        index = chip
        bit = 1
        while bit < chips:
            if m & bit:
                index = index + bit * (1 - 2 * ((chip // bit) % 2))
            bit *= 2
        return index

    def dev(m, c):
        return chip_xor(m) * 2 + c

    bits = [1 << i for i in range(chips.bit_length() - 1)]
    evens = [m for m in range(2, chips, 2)]
    top_bit = bits[-1]
    middle = bits[1:-1]
    q_paths = (bits[::-1], [top_bit, 1] + middle[::-1])
    o_paths = (None, None) * (HALF // 2)

    def q_hop(m, s):
        return [b for b in q_paths[s] if m & b][-1]

    def o_hop(m, j):
        if o_paths[j] is None:
            return 1 if m % 2 else m
        return [b for b in o_paths[j] if m & b][0]

    def o_children(m, j):
        return [x for x in range(1, chips) if x ^ o_hop(x, j) == m]


    def q_half(h):
        return pl.ds(pl.multiple_of(h * wide_cols, wide_cols), wide_cols)

    def kv_half(h):
        return pl.ds(pl.multiple_of(h * kv_cols, kv_cols), kv_cols)

    def token_half(h):
        return pl.ds(pl.multiple_of(h * tokens, tokens), tokens)

    def remote(src, dst, send, recv, where):
        return pltpu.make_async_remote_copy(
            src_ref=src, dst_ref=dst, send_sem=send, recv_sem=recv,
            device_id={"seq": where}, device_id_type=MESH,
        )

    q_copy = pltpu.make_async_copy(q_hbm, q_own, in_sem.at[0])
    q_mine = pltpu.make_async_copy(q_hbm.at[:, q_half(core)], qs.at[0, core], in_sem.at[1])
    k_mine = pltpu.make_async_copy(
        pk_hbm.at[:, kv_half(core)], pk.at[token_half(core)], in_sem.at[2])
    v_mine = pltpu.make_async_copy(
        pv_hbm.at[:, kv_half(core)], pv.at[token_half(core)], in_sem.at[3])
    small = [
        pltpu.make_async_copy(src, dst, in_sem.at[4 + i])
        for i, (src, dst) in enumerate((
            (nk_hbm, nk_ref), (nv_hbm, nv_ref), (table_hbm, table_ref), (pid_hbm, pid_ref)))
    ]
    q_copy.start()
    q_mine.start()
    for copy in small:
        copy.start()

    def suffix_copies(b):
        return (
            pltpu.make_async_copy(sk_hbm.at[b], sk.at[b], suf_sem.at[0, b]),
            pltpu.make_async_copy(sv_hbm.at[b], sv.at[b], suf_sem.at[1, b]),
        )

    barrier = pltpu.get_barrier_semaphore()
    peers = [dev(0, other)]
    for b in bits:
        peers += [dev(b, 0), dev(b, 1)]
    peers += [dev(m, core) for m in evens if m & (m - 1)]
    for peer in peers:
        pl.semaphore_signal(barrier, inc=1, device_id={"seq": peer}, device_id_type=MESH)
    for b in range(rows // 2):
        for copy in suffix_copies(b):
            copy.start()
    k_mine.start()
    v_mine.start()
    for b in range(rows // 2, rows):
        for copy in suffix_copies(b):
            copy.start()
    pl.semaphore_wait(barrier, len(peers))
    q_copy.wait()

    def own_copy(b, h):
        return remote(
            q_own.at[:, h * wide_cols:(h + 1) * wide_cols], qs.at[b, core],
            ag_send.at[b, h], ag_recv.at[b, core], dev(b, h))

    def forward_copy(m, s):
        hop = q_hop(m, s)
        return remote(
            qs.at[m ^ hop, s], qs.at[m, s], ag_send.at[m, s], ag_recv.at[m, s], dev(hop, core))

    partner_q = remote(
        q_own.at[:, q_half(other)], qs.at[0, core],
        ag_send.at[0, 0], ag_recv.at[0, 0], dev(0, other))
    partner_kv = [
        remote(src.at[:, kv_half(other)], dst.at[token_half(core)],
               kv_send.at[i], kv_recv.at[i], dev(0, other))
        for i, (src, dst) in enumerate(((pk_hbm, pk), (pv_hbm, pv)))
    ]

    for b in bits:
        for h in range(2):
            own_copy(b, h).start()
    partner_q.start()
    for copy in partner_kv:
        copy.start()

    arrived = set([(0, 0), (0, 1)])

    def pull(m, s):
        if (m, s) in arrived:
            return
        arrived.add((m, s))
        hop = q_hop(m, s)
        pull(m ^ hop, s)
        if m == hop:
            remote(
                q_own.at[:, 0:wide_cols], qs.at[m, s],
                ag_send.at[m, s], ag_recv.at[m, s], dev(m, core)).wait_recv()
        else:
            forward_copy(m, s).wait_recv()
        for b in reversed(q_paths[s][q_paths[s].index(hop) + 1:]):
            forward_copy(m | b, s).start()

    def arrive(m):
        for s in range(2):
            pull(m, s)

    for copy in small:
        copy.wait()

    for h in range(H):
        at = pl.ds(h, rows, stride=H)
        k = h // G
        q_rows[at, :] = q_own[:, h * HD:(h + 1) * HD].astype(jnp.float32)
        nk_rows[at, :] = nk_ref[:, k * HD:(k + 1) * HD].astype(jnp.float32)
        nv_rows[at, :] = nv_ref[:, k * HD:(k + 1) * HD].astype(jnp.float32)

    row_head = lax.broadcasted_iota(jnp.int32, (H, HD), 0) // G
    slot_iota = lax.broadcasted_iota(jnp.int32, (H, slots), 1)

    def suffix_scores(b):
        at = slice(b * H, (b + 1) * H)
        q = q_rows[at, :]
        wide = jnp.concatenate(
            [jnp.where(row_head == k, q, 0.0) for k in range(KV)], axis=1
        ).astype(jnp.bfloat16)
        s = lax.dot_general(wide, sk[b], NT, preferred_element_type=jnp.float32)
        s = jnp.where(slot_iota < lens_ref[b], s, MASKED)
        sn = jnp.sum(q * nk_rows[at, :], axis=1, keepdims=True)
        peak = jnp.maximum(jnp.max(s, axis=1, keepdims=True), sn)
        p = jnp.exp2((s - peak) * SCALE2)
        pn = jnp.exp2((sn - peak) * SCALE2)
        mass = jnp.sum(p, axis=1, keepdims=True) + pn
        weights[at, :] = p.astype(jnp.bfloat16)
        home_l[at, :] = jnp.broadcast_to(peak * SCALE2 + jnp.log2(mass), (H, HD))
        home_m[at, :] = jnp.broadcast_to(1.0 / mass, (H, HD))
        home_o[at, :] = pn * nv_rows[at, :]

    def suffix_outputs(b):
        at = slice(b * H, (b + 1) * H)
        o = jnp.dot(weights[at, :], sv[b], preferred_element_type=jnp.float32)
        own = home_o[at, :]
        for k in range(KV):
            own = own + jnp.where(row_head == k, o[:, k * HD:(k + 1) * HD], 0.0)
        home_o[at, :] = own * home_m[at, :]

    def suffix(first, last):
        for b in range(first, last):
            suffix_copies(b)[0].wait()
        for b in range(first, last):
            suffix_scores(b)
        for b in range(first, last):
            suffix_copies(b)[1].wait()
        for b in range(first, last):
            suffix_outputs(b)

    def prepare_labels():
        seqs = n * rows
        diag = (lax.broadcasted_iota(jnp.int32, (seqs, seqs), 0)
                == lax.broadcasted_iota(jnp.int32, (seqs, seqs), 1))
        pid = jnp.sum(jnp.where(diag, pid_ref[...].astype(jnp.float32), 0.0), axis=1, keepdims=True)
        lane = lax.broadcasted_iota(jnp.int32, (seqs, HD), 1).astype(jnp.float32)
        onehot[...] = jnp.where(lane == pid, 1.0, 0.0).astype(jnp.bfloat16)
        pages = 2 * tokens // page
        entries = table_ref.shape[1]
        ids = chip * pages + lax.broadcasted_iota(jnp.int32, (pages, entries), 0)
        page_lane = lax.broadcasted_iota(jnp.int32, (pages, HD), 1)
        bar = jnp.zeros((pages, HD), jnp.float32)
        for p in range(NPREF):
            hit = jnp.max(
                jnp.where(table_ref[p:p + 1, :] == ids, 1.0, 0.0), axis=1, keepdims=True)
            bar = jnp.where(page_lane == p, (1.0 - hit) * MASKED, bar)
        token = lax.broadcasted_iota(jnp.int32, (2 * tokens, pages), 0)
        first = lax.broadcasted_iota(jnp.int32, (2 * tokens, pages), 1) * page
        spread = jnp.where((token >= first) & (token < first + page), 1.0, 0.0)
        label[...] = jnp.dot(
            spread.astype(jnp.bfloat16), bar.astype(jnp.bfloat16),
            preferred_element_type=jnp.float32).astype(jnp.bfloat16)

    def prepare_values():
        v_mine.wait()
        partner_kv[1].wait_recv()
        for k in range(HALF):
            for t in starts:
                vt[k, :HD, t:t + step] = pv[t:t + step, k * HD:(k + 1) * HD].T
            vt[k, HD:, :] = jnp.ones((vt.shape[1] - HD, 2 * tokens), jnp.bfloat16)

    step = 256
    starts = range(0, 2 * tokens, step)

    def query_side(item):
        m, k = item
        parts = [(x, s) for x in (m, m + 1) for s in range(2)]
        code = jnp.concatenate(
            [onehot[pl.ds(pl.multiple_of(dev(x, s) * rows, rows), rows), :]
             for x, s in parts for g in range(G)], axis=0)
        q = jnp.concatenate(
            [qs[x, s, :, (k * G + g) * HD:(k * G + g + 1) * HD]
             for x, s in parts for g in range(G)], axis=0)
        return jnp.concatenate([q, code], axis=1)

    def advance(current, peak, following, slot):
        qx = None if following is None else query_side(following)
        top, o = None, None
        for t in starts:
            at = slice(t, t + step)
            if following is not None:
                k = following[1]
                kx = jnp.concatenate([pk[at, k * HD:(k + 1) * HD], label[at, :]], axis=1)
                s = lax.dot_general(kx, qx, NT, preferred_element_type=jnp.float32)
                scores[1 - slot, at, :] = s
                high = jnp.max(s, axis=0, keepdims=True)
                top = high if top is None else jnp.maximum(top, high)
            if current is not None:
                p = jnp.exp2((scores[slot, at, :] - peak) * SCALE2).astype(jnp.bfloat16)
                d = jnp.dot(vt[current[1], :, at], p, preferred_element_type=jnp.float32)
                o = d if o is None else o + d
        if current is not None:
            m, k = current
            mass = o[HD:HD + 1, :]
            res = (o[:HD, :] * (1.0 / mass)).astype(jnp.bfloat16)
            level = peak * SCALE2 + jnp.log2(mass)
            for x in range(2):
                part[m + x, k] = res[:, x * lanes:(x + 1) * lanes]
                lse[m + x, k] = level[:, x * lanes:(x + 1) * lanes]
        return top

    def part_copies(m, j):
        where = dev(o_hop(m, j), core)
        return [
            remote(part.at[m, j], near.at[m, j], o_send.at[m, j], o_recv.at[m, j], where),
            remote(lse.at[m, j], near_l.at[m, j], l_send.at[m, j], l_recv.at[m, j], where),
        ]

    def merge(m, child, j):
        for copy in part_copies(child, j):
            copy.wait_recv()
        la, lb = near_l[child, j], lse[m, j]
        w = 1.0 / (1.0 + jnp.exp2(lb - la))
        lse[m, j] = jnp.maximum(la, lb) + jnp.log2(1.0 + jnp.exp2(-jnp.abs(la - lb)))
        a = near[child, j].astype(jnp.float32)
        b = part[m, j].astype(jnp.float32)
        part[m, j] = (b + (a - b) * w).astype(jnp.bfloat16)

    def settle(m, j):
        for child in o_children(m, j):
            merge(m, child, j)
        if m:
            for copy in part_copies(m, j):
                copy.start()

    def split():
        pl.semaphore_signal(fence, 1)
        pl.semaphore_wait(fence, 1)

    ready, sent = set(), {}
    clock = [0]

    def depth(node):
        m, j = node
        return 0 if m == 0 else 1 + depth((m ^ o_hop(m, j), j))

    def progress(last):
        lag = 1 if last else 4
        for node in sorted(ready, key=lambda x: (-depth(x), -x[0], x[1])):
            if node[0] == 0 or (node[0] in () and not last):
                continue
            kids = [(c, node[1]) for c in o_children(*node)]
            if all(kid in sent and sent[kid] + lag <= clock[0] for kid in kids):
                settle(*node)
                ready.remove(node)
                sent[node] = clock[0]

    quarter = max(1, rows // 4)
    batches = list(range(0, rows, quarter))

    def fill(count):
        for _ in range(count):
            if batches:
                b = batches.pop(0)
                suffix(b, b + quarter)
                clock[0] += 2

    groups = [0, *evens[1:-1], 2, evens[-1]]
    prepare_labels()
    fill(1)
    arrive(groups[1])
    k_mine.wait()
    partner_kv[0].wait_recv()
    q_mine.wait()
    remote(q_own.at[:, 0:wide_cols], qs.at[0, other],
           ag_send.at[0, 0], ag_recv.at[0, 0], dev(0, other)).wait_recv()
    prepare_values()
    for x, m in enumerate(groups):
        if x == len(groups) - 1:
            fill(0)
        arrive(m)
        arrive(m + 1)
        peak = advance(None, None, (m, 0), 1)
        split()
        for k in range(HALF):
            peak = advance((m, k), peak, (m, k + 1) if k + 1 < HALF else None, k % 2)
            split()
            ready |= {(m, k), (m + 1, k)}
            progress(False)
            clock[0] += 1
            if k == 1 and x + 2 < len(groups):
                arrive(groups[x + 2])
    while batches:
        fill(1)
        progress(False)
    while len(sent) < HALF * (chips - 1):
        progress(True)
        clock[0] += 1
    for j in range(HALF):
        settle(0, j)
        fin[j] = part[0, j].astype(jnp.float32).T.astype(jnp.bfloat16)

    def column(src):
        levels = jnp.concatenate([src[k] for k in range(HALF)], axis=0)
        return jnp.concatenate([levels] * (HD // HALF), axis=0).T

    mine = rows * G
    give = remote(
        fin.at[:, pl.ds(pl.multiple_of(other * mine, mine), mine), :], got,
        f_send.at[0], f_recv.at[0], dev(0, other))
    give_l = remote(lse.at[0], got_l, f_send.at[1], f_recv.at[1], dev(0, other))
    give.start()
    give_l.start()

    def finish(half, levels, value):
        for k in range(HALF):
            j, i = k // (HALF // 2), k % (HALF // 2)
            for g in range(G):
                head = half * (HALF * G) + k * G + g
                level = levels[pl.ds(pl.multiple_of(core * mine + g * rows, rows), rows), k:k + 1]
                x = value(k, g).astype(jnp.float32)
                at = pl.ds(head, rows, stride=H)
                home = home_o[at, :]
                w = 1.0 / (1.0 + jnp.exp2(level - home_l[at, :]))
                out_ref[:, pl.ds(pl.multiple_of(head * HD, HD), HD)] = (
                    x + (home - x) * w).astype(jnp.bfloat16)

    cols[...] = column(lse.at[0])
    finish(core, cols, lambda k, g: fin[
        k, pl.ds(pl.multiple_of(core * mine + g * rows, rows), rows), :])
    give.wait_recv()
    give_l.wait_recv()
    cols_got[...] = column(got_l)
    finish(other, cols_got, lambda k, g: got[k, g * rows:(g + 1) * rows, :])

    for b in bits:
        for h in range(2):
            own_copy(b, h).wait_send()
    for m in range(1, chips):
        if m & (m - 1):
            for s in range(2):
                forward_copy(m, s).wait_send()
    partner_q.wait_send()
    for copy in partner_kv:
        copy.wait_send()
    for m in range(1, chips):
        for j in range(HALF):
            for copy in part_copies(m, j):
                copy.wait_send()
    give.wait_send()
    give_l.wait_send()


def local(
    queries, new_keys, new_values, suffix_keys, suffix_values, suffix_lens,
    prefix_keys, prefix_values, page_table, prefix_id,
):
    n = lax.axis_size("seq")
    chips = n // 2
    rows = queries.shape[0]
    slots = suffix_keys.shape[1]
    pages, page, width = prefix_keys.shape
    tokens = pages * page
    vmem = pl.BlockSpec(memory_space=pltpu.VMEM)
    hbm = pl.BlockSpec(memory_space=pl.ANY)
    smem = pl.BlockSpec(memory_space=pltpu.SMEM)
    bf16, f32 = jnp.bfloat16, jnp.float32
    dma = pltpu.SemaphoreType.DMA
    lanes = 2 * rows * G
    return pl.pallas_call(
        functools.partial(kernel, n, page),
        out_shape=jax.ShapeDtypeStruct((rows, H * HD), bf16),
        in_specs=[hbm, hbm, hbm, hbm, hbm, smem, hbm, hbm, hbm, hbm],
        out_specs=vmem,
        scratch_shapes=[
            pltpu.VMEM((rows, width), bf16),
            pltpu.VMEM((rows, width), bf16),
            pltpu.VMEM(page_table.shape, jnp.int32),
            pltpu.VMEM((1, n * rows), jnp.int32),
            pltpu.VMEM((rows, H * HD), bf16),
            pltpu.VMEM((chips, 2, rows, H * HD // 2), bf16),
            pltpu.VMEM((rows, slots, width), bf16),
            pltpu.VMEM((rows, slots, width), bf16),
            pltpu.VMEM((2 * tokens, width // 2), bf16),
            pltpu.VMEM((2 * tokens, width // 2), bf16),
            pltpu.VMEM((HALF, HD + 16, 2 * tokens), bf16),
            pltpu.VMEM((2 * tokens, HD), bf16),
            pltpu.VMEM((n * rows, HD), bf16),
            pltpu.VMEM((2, 2 * tokens, 2 * lanes), f32),
            pltpu.VMEM((chips, HALF, HD, lanes), bf16),
            pltpu.VMEM((chips, HALF, 1, lanes), f32),
            pltpu.VMEM((chips, HALF, HD, lanes), bf16),
            pltpu.VMEM((chips, HALF, 1, lanes), f32),
            pltpu.VMEM((HALF, lanes, HD), bf16),
            pltpu.VMEM((HALF, rows * G, HD), bf16),
            pltpu.VMEM((HALF, 1, lanes), f32),
            pltpu.VMEM((lanes, HD), f32),
            pltpu.VMEM((lanes, HD), f32),
            pltpu.VMEM((rows * H, HD), f32),
            pltpu.VMEM((rows * H, HD), f32),
            pltpu.VMEM((rows * H, HD), f32),
            pltpu.VMEM((rows * H, HD), f32),
            pltpu.VMEM((rows * H, HD), f32),
            pltpu.VMEM((rows * H, HD), f32),
            pltpu.VMEM((rows * H, slots), bf16),
            dma((8,)),
            pltpu.SemaphoreType.REGULAR,
            dma((2, rows)),
            dma((2,)), dma((2,)),
            dma((chips, 2)), dma((chips, 2)),
            dma((chips, HALF)), dma((chips, HALF)), dma((chips, HALF)), dma((chips, HALF)),
            dma((2,)), dma((2,)),
        ],
        compiler_params=pltpu.CompilerParams(
            collective_id=0, has_side_effects=True, vmem_limit_bytes=64 * 1024 * 1024 - 65536,
        ),
        name="step",
    )(
        queries, new_keys, new_values, suffix_keys, suffix_values, suffix_lens,
        prefix_keys.reshape(tokens, width), prefix_values.reshape(tokens, width),
        page_table, prefix_id.reshape(1, n * rows),
    )


def solution(mesh):
    return jax.shard_map(
        local,
        mesh=mesh,
        in_specs=(
            P(("grp", "seq"), None),
            P(("grp", "seq"), None),
            P(("grp", "seq"), None),
            P(("grp", "seq"), None, None),
            P(("grp", "seq"), None, None),
            P(("grp", "seq")),
            P(("grp", "seq"), None, None),
            P(("grp", "seq"), None, None),
            P("grp", None),
            P("grp"),
        ),
        out_specs=P(("grp", "seq"), None),
        check_vma=False,
    )
```
